32 devices in a mesh: row: 4 (over y, x), col: 8 (over z, core).
Axes of the slice: x: 2, y: 2, z: 4, core: 2. Of those that a mesh axis runs over, the one named last changes fastest.
Arguments:
- coeffs: bfloat16 [16384, 2048], P('row'), may hold values from -1 to 1
- p_slots: int32 [4, 8, 64], P('row', 'col'), may hold values from 0 to 511, as said below
- p_count: int32 [4, 8], P('row', 'col'), may hold values from 1 to 64
- s_blocks: bfloat16 [4, 8, 64, 128, 128], P('row', 'col'), may hold values from -0.3984375 to 0.3984375
- s_slots: int32 [4, 8, 64], P('row', 'col'), may hold values from 0 to 511, as said below
- s_count: int32 [4, 8], P('row', 'col'), may hold values from 1 to 64
- q_slots: int32 [4, 8, 64], P('row', 'col'), may hold values from 0 to 511, as said below
- q_count: int32 [4, 8], P('row', 'col'), may hold values from 1 to 64
Outputs:
- density: bfloat16 [4, 8, 64, 128, 128], P('row', 'col')
- product: float32 [4, 8, 64, 128, 128], P('row', 'col')
The draws below stay inside these ranges and needn't reach their ends.
Inputs may be any that keep to these rules, and one draw needn't show every extreme that they name: `p_slots`: on each device the live slots name different blocks of its tile; at least one device has all 64 slots live, which one is drawn. `s_slots`: on each device the live slots name different positions; at least one device has all 64 slots live, which one is drawn. `q_slots`: on each device the live slots name different blocks of its tile; at least one device has all 64 slots live, which one is drawn.
All inputs are finite; a program needn't handle non-finite values.
Results may differ from the reference program's by a relative error of at most 0.0029.
Values may be sent and summed in bfloat16 or wider, within the bound.
A program may use at most 192 MiB of HBM per device.

```python
import jax
import jax.numpy as jnp
from jax import lax

N = 16384
K = 2048
ROWB = 32
COLB = 16
SPAN = 2
PMAX = 64
QMAX = 64
SMAX = 64
N_ROW = 4
N_COL = 8


def pattern_slots(key, total, most):
    keys = jax.random.split(key, N_ROW * N_COL)
    picks = jax.vmap(lambda single: jax.random.permutation(single, total)[:most])(keys)
    return picks.reshape(N_ROW, N_COL, most).astype(jnp.int32)


def pattern_count(key, most):
    first_key, second_key = jax.random.split(key)
    counts = jax.random.randint(first_key, (N_ROW * N_COL,), 1, most + 1)
    chosen = jax.random.randint(second_key, (), 0, N_ROW * N_COL)
    counts = jnp.where(jnp.arange(N_ROW * N_COL) == chosen, most, counts)
    return counts.reshape(N_ROW, N_COL).astype(jnp.int32)


def draw_p_slots(key, part):
    return pattern_slots(jax.random.fold_in(key, 11), ROWB * COLB, PMAX)


def draw_p_count(key, part):
    return pattern_count(jax.random.fold_in(key, 12), PMAX)


def draw_s_slots(key, part):
    return pattern_slots(jax.random.fold_in(key, 21), SPAN * COLB * COLB, SMAX)


def draw_s_count(key, part):
    return pattern_count(jax.random.fold_in(key, 22), SMAX)


def draw_q_slots(key, part):
    return pattern_slots(jax.random.fold_in(key, 31), ROWB * COLB, QMAX)


def draw_q_count(key, part):
    return pattern_count(jax.random.fold_in(key, 32), QMAX)


def level_of(stream_key, shape, cuts, low, largest):
    def one(dim, blocks):
        steps = jax.random.uniform(jax.random.fold_in(jax.random.fold_in(stream_key, 6), dim), (blocks,), jnp.float32, low / len(cuts), largest / len(cuts))
        return jnp.repeat(jnp.exp(steps), shape[dim] // blocks).reshape((-1,) + (1,) * (len(shape) - dim - 1))

    gain = one(*cuts[0])
    for cut in cuts[1:]:
        gain = gain * one(*cut)
    return gain


def gaussian(own_key, extent, deviation, limit, shards=(), kind=jnp.bfloat16):
    array = jax.random.normal(own_key, extent, jnp.float32) * deviation
    if len(shards) > 0:
        array = level_of(own_key, extent, shards, -0.22, 0.18) * array
    return jnp.clip(array, min=-limit, max=limit).astype(kind)


def setup_inputs(seed: int = 0) -> dict:
    key_list = jax.random.split(jax.random.key(seed), 9)
    return {
        "coeffs": gaussian(key_list[0], (N, K), 0.15, 1.0, ((0, 4),)),
        "p_slots": draw_p_slots(jax.random.fold_in(key_list[8], 71), 0),
        "p_count": draw_p_count(jax.random.fold_in(key_list[8], 71), 0),
        "s_blocks": gaussian(key_list[3], (N_ROW, N_COL, SMAX, 128, 128), 0.0625, 0.3984375, ((0, 4), (1, 8))),
        "s_slots": draw_s_slots(jax.random.fold_in(key_list[8], 71), 0),
        "s_count": draw_s_count(jax.random.fold_in(key_list[8], 71), 0),
        "q_slots": draw_q_slots(jax.random.fold_in(key_list[8], 71), 0),
        "q_count": draw_q_count(jax.random.fold_in(key_list[8], 71), 0),
    }


def reference(coeffs, p_slots, p_count, s_blocks, s_slots, s_count, q_slots, q_count):
    block_count = coeffs.shape[0] // 128
    orbitals = coeffs.shape[1]
    tile_rows = block_count // N_ROW
    tile_cols = block_count // N_COL
    grid_row = jnp.arange(N_ROW, dtype=jnp.int32)[:, None, None]
    grid_col = jnp.arange(N_COL, dtype=jnp.int32)[None, :, None]
    blocked = coeffs.reshape(block_count, 128, orbitals)

    p_live = jnp.arange(p_slots.shape[2], dtype=jnp.int32)[None, None, :] < p_count[:, :, None]
    p_global_row = (grid_row * tile_rows + p_slots // tile_cols).astype(jnp.int32).reshape(-1)
    p_global_col = (grid_col * tile_cols + p_slots % tile_cols).astype(jnp.int32).reshape(-1)

    def density_block(pair):
        return jnp.dot(blocked[pair[0]], blocked[pair[1]].T, preferred_element_type=jnp.float32)

    raw = lax.map(density_block, (p_global_row, p_global_col))
    raw = raw.reshape(N_ROW, N_COL, -1, 128, 128)
    density = jnp.where(p_live[..., None, None], raw, jnp.zeros_like(raw)).astype(jnp.bfloat16)

    dense_p = jnp.zeros((block_count, block_count, 128, 128), jnp.bfloat16)
    dense_p = dense_p.at[p_global_row, p_global_col].add(density.reshape(-1, 128, 128))

    s_live = jnp.arange(s_slots.shape[2], dtype=jnp.int32)[None, None, :] < s_count[:, :, None]
    local_row = s_slots // tile_cols
    panel_index = grid_row + N_ROW * (local_row // tile_cols)
    s_global_row = (panel_index * tile_cols + local_row % tile_cols).astype(jnp.int32).reshape(-1)
    s_global_col = (grid_col * tile_cols + s_slots % tile_cols).astype(jnp.int32).reshape(-1)
    s_kept = jnp.where(s_live[..., None, None], s_blocks, jnp.zeros_like(s_blocks)).reshape(-1, 128, 128)
    dense_s = jnp.zeros((block_count, block_count, 128, 128), jnp.bfloat16)
    dense_s = dense_s.at[s_global_row, s_global_col].add(s_kept)

    q_live = jnp.arange(q_slots.shape[2], dtype=jnp.int32)[None, None, :] < q_count[:, :, None]
    q_global_row = (grid_row * tile_rows + q_slots // tile_cols).astype(jnp.int32).reshape(-1)
    q_global_col = (grid_col * tile_cols + q_slots % tile_cols).astype(jnp.int32).reshape(-1)

    def product_block(pair):
        left = dense_p[pair[0]].astype(jnp.float32)
        right = dense_s[:, pair[1]].astype(jnp.float32)
        return jnp.einsum('kab,kbc->ac', left, right)

    summed = lax.map(product_block, (q_global_row, q_global_col))
    summed = summed.reshape(N_ROW, N_COL, -1, 128, 128)
    product = jnp.where(q_live[..., None, None], summed, jnp.zeros_like(summed))
    return density, product
```

```python
import functools

import jax
import jax.numpy as jnp
from jax import lax
from jax.experimental import pallas as pl
from jax.experimental.pallas import tpu as pltpu
from jax.sharding import PartitionSpec as P

MESH = pl.DeviceIdType.MESH
MIB = 1 << 20


def rows_kernel(rows_n, cols_n, coeffs, out, send, recv):
    row, col = lax.axis_index("row"), lax.axis_index("col")
    sub = cols_n // rows_n
    height = out.shape[0]
    piece = height // rows_n
    half, share = lax.rem(col, sub), lax.div(col, sub)
    owner = lax.div(col, sub)
    targets = [
        {"row": lax.rem(row + step, rows_n), "col": row * sub + half} for step in range(1, rows_n)
    ]
    sources = [{"row": owner, "col": part * sub + half} for part in range(rows_n)]
    barrier = pltpu.get_barrier_semaphore()
    for device in targets:
        pl.semaphore_signal(barrier, inc=1, device_id=device, device_id_type=MESH)

    @pl.when(row != owner)
    def _():
        for device in sources:
            pl.semaphore_signal(barrier, inc=1, device_id=device, device_id_type=MESH)

    pl.semaphore_wait(barrier, rows_n - 1 + jnp.where(row != owner, rows_n, 0))

    def copy(step, part, device):
        start = half * height + share * piece
        return pltpu.make_async_remote_copy(
            src_ref=coeffs.at[pl.ds(pl.multiple_of(start, piece), piece)],
            dst_ref=out.at[pl.ds(pl.multiple_of(part * piece, piece), piece)],
            send_sem=send.at[step],
            recv_sem=recv.at[part],
            device_id=device,
            device_id_type=MESH,
        )

    sends = [copy(step, share, device) for step, device in enumerate(targets)]
    for one in sends:
        one.start()

    @pl.when(row != owner)
    def _():
        for part, device in enumerate(sources):
            copy(0, part, device).wait_recv()

    for one in sends:
        one.wait_send()


def gather_rows(coeffs, rows_n, cols_n):
    height = coeffs.shape[0] * rows_n // cols_n
    return pl.pallas_call(
        functools.partial(rows_kernel, rows_n, cols_n),
        out_shape=jax.ShapeDtypeStruct((height, coeffs.shape[1]), coeffs.dtype),
        in_specs=[pl.BlockSpec(memory_space=pl.ANY)],
        out_specs=pl.BlockSpec(memory_space=pl.ANY),
        scratch_shapes=[
            pltpu.SemaphoreType.DMA((rows_n - 1,)),
            pltpu.SemaphoreType.DMA((rows_n,)),
        ],
        compiler_params=pltpu.CompilerParams(collective_id=0, has_side_effects=True),
    )(coeffs)


def density_kernel(rows_n, cols_n, ids, count, coeffs, others, out, left, right, sem):
    row, col = lax.axis_index("row"), lax.axis_index("col")
    sub = cols_n // rows_n
    height = others.shape[0]
    tile_cols = height // 128
    load_left = pltpu.make_async_copy(coeffs, left, sem.at[0])
    load_left.start()
    here = row == lax.div(col, sub)
    start = pl.multiple_of(lax.rem(col, sub) * height, height)
    load_own = pltpu.make_async_copy(coeffs.at[pl.ds(start, height)], right, sem.at[1])
    load_other = pltpu.make_async_copy(others, right, sem.at[1])

    @pl.when(here)
    def _():
        load_own.start()

    @pl.when(jnp.logical_not(here))
    def _():
        load_other.start()

    live = count[0]
    load_left.wait()
    load_other.wait()

    def block(slot, carry):
        a = pl.multiple_of(lax.div(ids[slot], tile_cols) * 128, 128)
        b = pl.multiple_of(lax.rem(ids[slot], tile_cols) * 128, 128)
        raw = lax.dot_general(
            left[pl.ds(a, 128), :],
            right[pl.ds(b, 128), :],
            (((1,), (1,)), ((), ())),
            preferred_element_type=jnp.float32,
        )
        out[slot] = raw.astype(out.dtype)
        return carry

    def clear(slot, carry):
        out[slot] = jnp.zeros(out.shape[1:], out.dtype)
        return carry

    lax.fori_loop(0, live, block, 0)
    lax.fori_loop(live, out.shape[0], clear, 0)


def density(ids, count, coeffs, others, rows_n, cols_n):
    slots = ids.shape[0]
    return pl.pallas_call(
        functools.partial(density_kernel, rows_n, cols_n),
        out_shape=jax.ShapeDtypeStruct((slots, 128, 128), jnp.bfloat16),
        in_specs=[pl.BlockSpec(memory_space=pltpu.SMEM)] * 2
        + [pl.BlockSpec(memory_space=pl.ANY)] * 2,
        out_specs=pl.BlockSpec(memory_space=pltpu.VMEM),
        scratch_shapes=[
            pltpu.VMEM(coeffs.shape, coeffs.dtype),
            pltpu.VMEM(others.shape, coeffs.dtype),
            pltpu.SemaphoreType.DMA((2,)),
        ],
        compiler_params=pltpu.CompilerParams(vmem_limit_bytes=40 * MIB),
    )(ids, count, coeffs, others)


def blocks_kernel(rows_n, cols_n, parts, p_own, s_own, p_all, s_all, *sems):
    send, recv, pass_send, pass_recv, s_send, s_recv = sems
    row, col = lax.axis_index("row"), lax.axis_index("col")
    length = cols_n // 2
    z, core = lax.div(col, 2), lax.rem(col, 2)
    size = p_own.shape[0] // parts
    right, left = {"row": row, "col": col + 2}, {"row": row, "col": col - 2}
    partner = {"row": row, "col": z * 2 + 1 - core}
    column = [{"row": lax.rem(row + step, rows_n), "col": col} for step in range(1, rows_n)]
    has_right, has_left = z + 1 < length, z > 0

    barrier = pltpu.get_barrier_semaphore()

    def greet(device):
        pl.semaphore_signal(barrier, inc=1, device_id=device, device_id_type=MESH)

    greet(partner)
    for device in column:
        greet(device)

    @pl.when(has_right)
    def _():
        greet(right)

    @pl.when(has_left)
    def _():
        greet(left)

    pl.semaphore_wait(barrier, rows_n + jnp.where(has_right, 1, 0) + jnp.where(has_left, 1, 0))

    def remote(src, dst, send_sem, recv_sem, device):
        return pltpu.make_async_remote_copy(
            src_ref=src,
            dst_ref=dst,
            send_sem=send_sem,
            recv_sem=recv_sem,
            device_id=device,
            device_id_type=MESH,
        )

    def piece(source, lane, part):
        return p_all.at[source * 2 + lane, pl.ds(part * size, size)]

    def origin(way, step):
        return z - step if way == 0 else z + step

    def sent(way, step, part):
        where = piece(origin(way, step), core, part)
        src = p_own.at[pl.ds(part * size, size)] if step == 0 else where
        device = right if way == 0 else left
        return remote(src, where, send.at[way, step, part], recv.at[way, step, part], device)

    def passed(way, step, part):
        where = piece(origin(way, step), core, part)
        src = p_own.at[pl.ds(part * size, size)] if step == 0 else where
        return remote(
            src, where, pass_send.at[way, step, part], pass_recv.at[way, step, part], partner
        )

    def onward(way):
        return has_right if way == 0 else has_left

    def exists(way, step):
        return z >= step if way == 0 else z + step < length

    for part in range(parts):
        for way in range(2):
            pl.when(onward(way))(lambda way=way: sent(way, 0, part).start())
    s_sends = [
        remote(s_own, s_all.at[row], s_send.at[n], s_recv.at[n], device)
        for n, device in enumerate(column)
    ]
    for one in s_sends:
        one.start()
    for part in range(parts):
        passed(0, 0, part).start()
    for step in range(1, length):
        for part in range(parts):
            for way in range(2):

                @pl.when(exists(way, step))
                def _():
                    sent(way, step - 1, part).wait_recv()
                    passed(way, step, part).start()
                    if step < length - 1:
                        pl.when(onward(way))(lambda: sent(way, step, part).start())

    for part in range(parts):
        passed(0, 0, part).wait()
        for way in range(2):
            pl.when(onward(way))(lambda way=way: sent(way, 0, part).wait_send())
    for step in range(1, length):
        for part in range(parts):
            for way in range(2):

                @pl.when(exists(way, step))
                def _():
                    passed(way, step, part).wait()
                    if step < length - 1:
                        pl.when(onward(way))(lambda: sent(way, step, part).wait_send())

    for one in s_sends:
        one.wait()


def gather_blocks(p_own, s_own, rows_n, cols_n):
    parts = 4 if p_own.shape[0] % 4 == 0 else 1
    table = pltpu.SemaphoreType.DMA((2, cols_n // 2, parts))
    return pl.pallas_call(
        functools.partial(blocks_kernel, rows_n, cols_n, parts),
        out_shape=(
            jax.ShapeDtypeStruct((cols_n,) + p_own.shape, p_own.dtype),
            jax.ShapeDtypeStruct((rows_n,) + s_own.shape, s_own.dtype),
        ),
        in_specs=[pl.BlockSpec(memory_space=pl.ANY)] * 2,
        out_specs=[pl.BlockSpec(memory_space=pl.ANY)] * 2,
        scratch_shapes=[table] * 4 + [pltpu.SemaphoreType.DMA((rows_n - 1,))] * 2,
        compiler_params=pltpu.CompilerParams(collective_id=1, has_side_effects=True),
    )(p_own, s_own)


def product_kernel(rows_n, cols_n, codes, counts, p_own, s_own, p_all, s_all, out, left, right, sem):
    row, col = lax.axis_index("row"), lax.axis_index("col")
    p_max, s_max = p_own.shape[0], s_own.shape[0]
    base = rows_n * s_max
    loads = [pltpu.make_async_copy(p_own, left.at[pl.ds(col * p_max, p_max)], sem.at[0])]
    loads += [pltpu.make_async_copy(s_own, right.at[pl.ds(row * s_max, s_max)], sem.at[1])]
    for step in range(1, cols_n):
        at = lax.rem(col + step, cols_n)
        loads += [
            pltpu.make_async_copy(
                p_all.at[at], left.at[pl.ds(at * p_max, p_max)], sem.at[len(loads)]
            )
        ]
    for step in range(1, rows_n):
        at = lax.rem(row + step, rows_n)
        loads += [
            pltpu.make_async_copy(
                s_all.at[at], right.at[pl.ds(at * s_max, s_max)], sem.at[len(loads)]
            )
        ]
    for load in loads:
        load.start()
    for load in loads:
        load.wait()

    def slot(q, carry):
        def term(n, total):
            code = codes[q, n]
            return total + jnp.dot(
                left[lax.div(code, base)],
                right[lax.rem(code, base)],
                preferred_element_type=jnp.float32,
            )

        out[q] = lax.fori_loop(0, counts[q], term, jnp.zeros((128, 128), jnp.float32))
        return carry

    lax.fori_loop(0, out.shape[0], slot, 0)


def block_product(codes, counts, p_own, s_own, p_all, s_all):
    cols_n, p_max = p_all.shape[:2]
    rows_n, s_max = s_all.shape[:2]
    return pl.pallas_call(
        functools.partial(product_kernel, rows_n, cols_n),
        out_shape=jax.ShapeDtypeStruct((counts.shape[0], 128, 128), jnp.float32),
        in_specs=[pl.BlockSpec(memory_space=pltpu.SMEM)] * 2
        + [pl.BlockSpec(memory_space=pl.ANY)] * 4,
        out_specs=pl.BlockSpec(memory_space=pltpu.VMEM),
        scratch_shapes=[
            pltpu.VMEM((cols_n * p_max, 128, 128), p_all.dtype),
            pltpu.VMEM((rows_n * s_max, 128, 128), s_all.dtype),
            pltpu.SemaphoreType.DMA((cols_n + rows_n,)),
        ],
        compiler_params=pltpu.CompilerParams(vmem_limit_bytes=40 * MIB),
    )(codes, counts, p_own, s_own, p_all, s_all)


def match_lists(p_codes, s_codes, q_ids, q_live, tile_cols, span):
    cols_n, p_max = p_codes.shape
    rows_n, s_max = s_codes.shape
    q_row, q_col = q_ids // tile_cols, q_ids % tile_cols
    at = jnp.arange(tile_cols, dtype=jnp.int32)
    p_want = q_row[:, None] * tile_cols + at[None, :]
    p_hit = p_codes[None, :, None, :] == p_want[:, None, :, None]
    p_slot = jnp.arange(cols_n * p_max, dtype=jnp.int32).reshape(1, cols_n, 1, p_max)
    p_at = jnp.max(jnp.where(p_hit, p_slot, -1), axis=3)
    level = jnp.arange(span * tile_cols, dtype=jnp.int32).reshape(span, tile_cols)
    s_want = level[None] * tile_cols + q_col[:, None, None]
    s_hit = s_codes[None, None, :, None, :] == s_want[:, :, None, :, None]
    s_slot = jnp.arange(rows_n * s_max, dtype=jnp.int32).reshape(1, 1, rows_n, 1, s_max)
    s_at = jnp.max(jnp.where(s_hit, s_slot, -1), axis=4)
    p_at = p_at.reshape(q_ids.shape[0], -1)
    s_at = s_at.reshape(q_ids.shape[0], -1)
    depth = p_at.shape[1]
    match = (p_at >= 0) & (s_at >= 0) & q_live[:, None]
    code = jnp.where(match, p_at * (rows_n * s_max) + s_at, 0)
    order = jnp.arange(depth, dtype=jnp.int32)
    before = order[None, :, None] > order[None, None, :]
    rank = jnp.sum((before & match[:, None, :]).astype(jnp.int32), axis=2)
    rank = jnp.where(match, rank, -1)
    picked = rank[:, None, :] == order[None, :, None]
    codes = jnp.sum(jnp.where(picked, code[:, None, :], 0), axis=2)
    return codes, jnp.sum(match.astype(jnp.int32), axis=1)


def on_device(coeffs, p_slots, p_count, s_blocks, s_slots, s_count, q_slots, q_count):
    rows_n = lax.axis_size("row")
    cols_n = lax.axis_size("col")
    tile_cols = coeffs.shape[0] * rows_n // cols_n // 128
    p_ids, s_ids, q_ids = p_slots[0, 0], s_slots[0, 0], q_slots[0, 0]
    s_own = s_blocks[0, 0]
    p_max, s_max, q_max = p_ids.shape[0], s_ids.shape[0], q_ids.shape[0]

    def live(ids, count):
        return jnp.arange(ids.shape[0], dtype=jnp.int32) < count[0, 0]

    p_codes = lax.all_gather(jnp.where(live(p_ids, p_count), p_ids, -1), "col")
    s_codes = lax.all_gather(jnp.where(live(s_ids, s_count), s_ids, -1), "row")
    codes, counts = match_lists(
        p_codes, s_codes, q_ids, live(q_ids, q_count), tile_cols, cols_n // rows_n
    )
    others = gather_rows(coeffs, rows_n, cols_n)
    p_own = density(p_ids, p_count[0], coeffs, others, rows_n, cols_n)
    p_all, s_all = gather_blocks(p_own, s_own, rows_n, cols_n)
    product = block_product(codes, counts, p_own, s_own, p_all, s_all)
    return (p_own.reshape(1, 1, p_max, 128, 128), product.reshape(1, 1, q_max, 128, 128))


def solution(mesh):
    return jax.shard_map(
        on_device,
        mesh=mesh,
        in_specs=(
            P("row", None),
            P("row", "col", None),
            P("row", "col"),
            P("row", "col", None, None, None),
            P("row", "col", None),
            P("row", "col"),
            P("row", "col", None),
            P("row", "col"),
        ),
        out_specs=(P("row", "col", None, None, None), P("row", "col", None, None, None)),
        check_vma=False,
    )
```

```python
import functools

import jax
import jax.numpy as jnp
from jax import lax
from jax.experimental import pallas as pl
from jax.experimental.pallas import tpu as pltpu
from jax.sharding import PartitionSpec as P

MESH = pl.DeviceIdType.MESH
MIB = 1 << 20


def rows_kernel(rows_n, cols_n, coeffs, out, send, recv):
    row, col = lax.axis_index("row"), lax.axis_index("col")
    sub = cols_n // rows_n
    height = out.shape[0]
    piece = height // rows_n
    half, share = lax.rem(col, sub), lax.div(col, sub)
    owner = lax.div(col, sub)
    targets = [
        {"row": lax.rem(row + step, rows_n), "col": row * sub + half} for step in range(1, rows_n)
    ]
    sources = [{"row": owner, "col": part * sub + half} for part in range(rows_n)]
    barrier = pltpu.get_barrier_semaphore()
    for device in targets:
        pl.semaphore_signal(barrier, inc=1, device_id=device, device_id_type=MESH)

    @pl.when(row != owner)
    def _():
        for device in sources:
            pl.semaphore_signal(barrier, inc=1, device_id=device, device_id_type=MESH)

    pl.semaphore_wait(barrier, rows_n - 1 + jnp.where(row != owner, rows_n, 0))

    def copy(step, part, device):
        start = half * height + share * piece
        return pltpu.make_async_remote_copy(
            src_ref=coeffs.at[pl.ds(pl.multiple_of(start, piece), piece)],
            dst_ref=out.at[pl.ds(pl.multiple_of(part * piece, piece), piece)],
            send_sem=send.at[step],
            recv_sem=recv.at[part],
            device_id=device,
            device_id_type=MESH,
        )

    sends = [copy(step, share, device) for step, device in enumerate(targets)]
    for one in sends:
        one.start()

    @pl.when(row != owner)
    def _():
        for part, device in enumerate(sources):
            copy(0, part, device).wait_recv()

    for one in sends:
        one.wait_send()


def square_kernel(rows_n, cols_n, parts, coeffs, out, send, recv):
    row, col = lax.axis_index("row"), lax.axis_index("col")
    sub = cols_n // rows_n
    height = out.shape[0]
    size = height // (2 * parts)
    owner = lax.div(col, sub)
    first = lax.rem(col, sub) * height
    y, x = lax.div(row, 2), lax.rem(row, 2)
    dy = lax.rem(y + lax.div(owner, 2), 2)
    dx = lax.rem(x + lax.rem(owner, 2), 2)
    along_x, along_y = y * 2 + 1 - x, (1 - y) * 2 + x
    is_source = row == owner
    sends = [jnp.logical_or(dx == 1, dy == 0), jnp.logical_or(dx == 0, dy == 1)]
    following = [
        jnp.where(dx == dy, along_x, along_y),
        jnp.where(dx == dy, along_y, along_x),
    ]

    barrier = pltpu.get_barrier_semaphore()
    for near in (along_x, along_y):
        pl.semaphore_signal(
            barrier, inc=1, device_id={"row": near, "col": col}, device_id_type=MESH
        )
    pl.semaphore_wait(barrier, 2)

    def copy(way, part, from_input):
        offset = (way * parts + part) * size
        where = out.at[pl.ds(offset, size)]
        start = pl.multiple_of(first + offset, size)
        return pltpu.make_async_remote_copy(
            src_ref=coeffs.at[pl.ds(start, size)] if from_input else where,
            dst_ref=where,
            send_sem=send.at[way, part],
            recv_sem=recv.at[way, part],
            device_id={"row": following[way], "col": col},
            device_id_type=MESH,
        )

    @pl.when(is_source)
    def _():
        for part in range(parts):
            for way in range(2):
                copy(way, part, True).start()

    @pl.when(jnp.logical_not(is_source))
    def _():
        for part in range(parts):
            for way in range(2):
                copy(way, part, False).wait_recv()
                pl.when(sends[way])(lambda: copy(way, part, False).start())

    for way in range(2):

        @pl.when(sends[way])
        def _():
            for part in range(parts):
                copy(way, part, False).wait_send()


def gather_rows(coeffs, rows_n, cols_n):
    height = coeffs.shape[0] * rows_n // cols_n
    if rows_n == 4:
        parts = max(1, height // 256)
        body = functools.partial(square_kernel, rows_n, cols_n, parts)
        sems = [pltpu.SemaphoreType.DMA((2, parts))] * 2
    else:
        body = functools.partial(rows_kernel, rows_n, cols_n)
        sems = [pltpu.SemaphoreType.DMA((rows_n - 1,)), pltpu.SemaphoreType.DMA((rows_n,))]
    return pl.pallas_call(
        body,
        out_shape=jax.ShapeDtypeStruct((height, coeffs.shape[1]), coeffs.dtype),
        in_specs=[pl.BlockSpec(memory_space=pl.ANY)],
        out_specs=pl.BlockSpec(memory_space=pl.ANY),
        scratch_shapes=sems,
        compiler_params=pltpu.CompilerParams(collective_id=0, has_side_effects=True),
    )(coeffs)


def density_kernel(rows_n, cols_n, ids, count, coeffs, others, out, left, right, sem):
    row, col = lax.axis_index("row"), lax.axis_index("col")
    sub = cols_n // rows_n
    height = others.shape[0]
    tile_cols = height // 128
    load_left = pltpu.make_async_copy(coeffs, left, sem.at[0])
    load_left.start()
    here = row == lax.div(col, sub)
    start = pl.multiple_of(lax.rem(col, sub) * height, height)
    load_own = pltpu.make_async_copy(coeffs.at[pl.ds(start, height)], right, sem.at[1])
    load_other = pltpu.make_async_copy(others, right, sem.at[1])

    @pl.when(here)
    def _():
        load_own.start()

    @pl.when(jnp.logical_not(here))
    def _():
        load_other.start()

    live = count[0]
    load_left.wait()
    load_other.wait()

    def block(slot, carry):
        a = pl.multiple_of(lax.div(ids[slot], tile_cols) * 128, 128)
        b = pl.multiple_of(lax.rem(ids[slot], tile_cols) * 128, 128)
        raw = lax.dot_general(
            left[pl.ds(a, 128), :],
            right[pl.ds(b, 128), :],
            (((1,), (1,)), ((), ())),
            preferred_element_type=jnp.float32,
        )
        out[slot] = raw.astype(out.dtype)
        return carry

    def clear(slot, carry):
        out[slot] = jnp.zeros(out.shape[1:], out.dtype)
        return carry

    lax.fori_loop(0, live, block, 0)
    lax.fori_loop(live, out.shape[0], clear, 0)


def density(ids, count, coeffs, others, rows_n, cols_n):
    slots = ids.shape[0]
    return pl.pallas_call(
        functools.partial(density_kernel, rows_n, cols_n),
        out_shape=jax.ShapeDtypeStruct((slots, 128, 128), jnp.bfloat16),
        in_specs=[pl.BlockSpec(memory_space=pltpu.SMEM)] * 2
        + [pl.BlockSpec(memory_space=pl.ANY)] * 2,
        out_specs=pl.BlockSpec(memory_space=pltpu.VMEM),
        scratch_shapes=[
            pltpu.VMEM(coeffs.shape, coeffs.dtype),
            pltpu.VMEM(others.shape, coeffs.dtype),
            pltpu.SemaphoreType.DMA((2,)),
        ],
        compiler_params=pltpu.CompilerParams(vmem_limit_bytes=40 * MIB),
    )(ids, count, coeffs, others)


def blocks_kernel(rows_n, cols_n, parts, p_own, s_own, p_all, s_all, *sems):
    send, recv, pass_send, pass_recv, s_send, s_recv = sems
    row, col = lax.axis_index("row"), lax.axis_index("col")
    length = cols_n // 2
    z, core = lax.div(col, 2), lax.rem(col, 2)
    size = p_own.shape[0] // parts
    right, left = {"row": row, "col": col + 2}, {"row": row, "col": col - 2}
    partner = {"row": row, "col": z * 2 + 1 - core}
    column = [{"row": lax.rem(row + step, rows_n), "col": col} for step in range(1, rows_n)]
    has_right, has_left = z + 1 < length, z > 0

    barrier = pltpu.get_barrier_semaphore()

    def greet(device):
        pl.semaphore_signal(barrier, inc=1, device_id=device, device_id_type=MESH)

    greet(partner)
    for device in column:
        greet(device)

    @pl.when(has_right)
    def _():
        greet(right)

    @pl.when(has_left)
    def _():
        greet(left)

    pl.semaphore_wait(barrier, rows_n + jnp.where(has_right, 1, 0) + jnp.where(has_left, 1, 0))

    def remote(src, dst, send_sem, recv_sem, device):
        return pltpu.make_async_remote_copy(
            src_ref=src,
            dst_ref=dst,
            send_sem=send_sem,
            recv_sem=recv_sem,
            device_id=device,
            device_id_type=MESH,
        )

    def piece(source, lane, part):
        return p_all.at[source * 2 + lane, pl.ds(part * size, size)]

    def origin(way, step):
        return z - step if way == 0 else z + step

    def sent(way, step, part):
        where = piece(origin(way, step), core, part)
        src = p_own.at[pl.ds(part * size, size)] if step == 0 else where
        device = right if way == 0 else left
        return remote(src, where, send.at[way, step, part], recv.at[way, step, part], device)

    def passed(way, step, part):
        where = piece(origin(way, step), core, part)
        src = p_own.at[pl.ds(part * size, size)] if step == 0 else where
        return remote(
            src, where, pass_send.at[way, step, part], pass_recv.at[way, step, part], partner
        )

    def onward(way):
        return has_right if way == 0 else has_left

    def exists(way, step):
        return z >= step if way == 0 else z + step < length

    for part in range(parts):
        for way in range(2):
            pl.when(onward(way))(lambda way=way: sent(way, 0, part).start())
    s_sends = [
        remote(s_own, s_all.at[row], s_send.at[n], s_recv.at[n], device)
        for n, device in enumerate(column)
    ]
    for one in s_sends:
        one.start()
    for part in range(parts):
        passed(0, 0, part).start()
    for step in range(1, length):
        for part in range(parts):
            for way in range(2):

                @pl.when(exists(way, step))
                def _():
                    sent(way, step - 1, part).wait_recv()
                    passed(way, step, part).start()
                    if step < length - 1:
                        pl.when(onward(way))(lambda: sent(way, step, part).start())

    for part in range(parts):
        passed(0, 0, part).wait()
        for way in range(2):
            pl.when(onward(way))(lambda way=way: sent(way, 0, part).wait_send())
    for step in range(1, length):
        for part in range(parts):
            for way in range(2):

                @pl.when(exists(way, step))
                def _():
                    passed(way, step, part).wait()
                    if step < length - 1:
                        pl.when(onward(way))(lambda: sent(way, step, part).wait_send())

    for one in s_sends:
        one.wait()


def gather_blocks(p_own, s_own, rows_n, cols_n):
    parts = 4 if p_own.shape[0] % 4 == 0 else 1
    table = pltpu.SemaphoreType.DMA((2, cols_n // 2, parts))
    return pl.pallas_call(
        functools.partial(blocks_kernel, rows_n, cols_n, parts),
        out_shape=(
            jax.ShapeDtypeStruct((cols_n,) + p_own.shape, p_own.dtype),
            jax.ShapeDtypeStruct((rows_n,) + s_own.shape, s_own.dtype),
        ),
        in_specs=[pl.BlockSpec(memory_space=pl.ANY)] * 2,
        out_specs=[pl.BlockSpec(memory_space=pl.ANY)] * 2,
        scratch_shapes=[table] * 4 + [pltpu.SemaphoreType.DMA((rows_n - 1,))] * 2,
        compiler_params=pltpu.CompilerParams(collective_id=1, has_side_effects=True),
    )(p_own, s_own)


def product_kernel(rows_n, cols_n, codes, counts, p_own, s_own, p_all, s_all, out, left, right, sem):
    row, col = lax.axis_index("row"), lax.axis_index("col")
    p_max, s_max = p_own.shape[0], s_own.shape[0]
    base = rows_n * s_max
    loads = [pltpu.make_async_copy(p_own, left.at[pl.ds(col * p_max, p_max)], sem.at[0])]
    loads += [pltpu.make_async_copy(s_own, right.at[pl.ds(row * s_max, s_max)], sem.at[1])]
    for step in range(1, cols_n):
        at = lax.rem(col + step, cols_n)
        loads += [
            pltpu.make_async_copy(
                p_all.at[at], left.at[pl.ds(at * p_max, p_max)], sem.at[len(loads)]
            )
        ]
    for step in range(1, rows_n):
        at = lax.rem(row + step, rows_n)
        loads += [
            pltpu.make_async_copy(
                s_all.at[at], right.at[pl.ds(at * s_max, s_max)], sem.at[len(loads)]
            )
        ]
    for load in loads:
        load.start()
    for load in loads:
        load.wait()

    def slot(q, carry):
        def term(n, total):
            code = codes[q, n]
            return total + jnp.dot(
                left[lax.div(code, base)],
                right[lax.rem(code, base)],
                preferred_element_type=jnp.float32,
            )

        out[q] = lax.fori_loop(0, counts[q], term, jnp.zeros((128, 128), jnp.float32))
        return carry

    lax.fori_loop(0, out.shape[0], slot, 0)


def block_product(codes, counts, p_own, s_own, p_all, s_all):
    cols_n, p_max = p_all.shape[:2]
    rows_n, s_max = s_all.shape[:2]
    return pl.pallas_call(
        functools.partial(product_kernel, rows_n, cols_n),
        out_shape=jax.ShapeDtypeStruct((counts.shape[0], 128, 128), jnp.float32),
        in_specs=[pl.BlockSpec(memory_space=pltpu.SMEM)] * 2
        + [pl.BlockSpec(memory_space=pl.ANY)] * 4,
        out_specs=pl.BlockSpec(memory_space=pltpu.VMEM),
        scratch_shapes=[
            pltpu.VMEM((cols_n * p_max, 128, 128), p_all.dtype),
            pltpu.VMEM((rows_n * s_max, 128, 128), s_all.dtype),
            pltpu.SemaphoreType.DMA((cols_n + rows_n,)),
        ],
        compiler_params=pltpu.CompilerParams(vmem_limit_bytes=40 * MIB),
    )(codes, counts, p_own, s_own, p_all, s_all)


def match_lists(p_codes, s_codes, q_ids, q_live, tile_cols, span):
    cols_n, p_max = p_codes.shape
    rows_n, s_max = s_codes.shape
    q_row, q_col = q_ids // tile_cols, q_ids % tile_cols
    at = jnp.arange(tile_cols, dtype=jnp.int32)
    p_want = q_row[:, None] * tile_cols + at[None, :]
    p_hit = p_codes[None, :, None, :] == p_want[:, None, :, None]
    p_slot = jnp.arange(cols_n * p_max, dtype=jnp.int32).reshape(1, cols_n, 1, p_max)
    p_at = jnp.max(jnp.where(p_hit, p_slot, -1), axis=3)
    level = jnp.arange(span * tile_cols, dtype=jnp.int32).reshape(span, tile_cols)
    s_want = level[None] * tile_cols + q_col[:, None, None]
    s_hit = s_codes[None, None, :, None, :] == s_want[:, :, None, :, None]
    s_slot = jnp.arange(rows_n * s_max, dtype=jnp.int32).reshape(1, 1, rows_n, 1, s_max)
    s_at = jnp.max(jnp.where(s_hit, s_slot, -1), axis=4)
    p_at = p_at.reshape(q_ids.shape[0], -1)
    s_at = s_at.reshape(q_ids.shape[0], -1)
    depth = p_at.shape[1]
    match = (p_at >= 0) & (s_at >= 0) & q_live[:, None]
    code = jnp.where(match, p_at * (rows_n * s_max) + s_at, 0)
    order = jnp.arange(depth, dtype=jnp.int32)
    before = order[None, :, None] > order[None, None, :]
    rank = jnp.sum((before & match[:, None, :]).astype(jnp.int32), axis=2)
    rank = jnp.where(match, rank, -1)
    picked = rank[:, None, :] == order[None, :, None]
    codes = jnp.sum(jnp.where(picked, code[:, None, :], 0), axis=2)
    return codes, jnp.sum(match.astype(jnp.int32), axis=1)


def on_device(coeffs, p_slots, p_count, s_blocks, s_slots, s_count, q_slots, q_count):
    rows_n = lax.axis_size("row")
    cols_n = lax.axis_size("col")
    tile_cols = coeffs.shape[0] * rows_n // cols_n // 128
    p_ids, s_ids, q_ids = p_slots[0, 0], s_slots[0, 0], q_slots[0, 0]
    s_own = s_blocks[0, 0]
    p_max, s_max, q_max = p_ids.shape[0], s_ids.shape[0], q_ids.shape[0]

    def live(ids, count):
        return jnp.arange(ids.shape[0], dtype=jnp.int32) < count[0, 0]

    p_codes = lax.all_gather(jnp.where(live(p_ids, p_count), p_ids, -1), "col")
    s_codes = lax.all_gather(jnp.where(live(s_ids, s_count), s_ids, -1), "row")
    codes, counts = match_lists(
        p_codes, s_codes, q_ids, live(q_ids, q_count), tile_cols, cols_n // rows_n
    )
    others = gather_rows(coeffs, rows_n, cols_n)
    p_own = density(p_ids, p_count[0], coeffs, others, rows_n, cols_n)
    p_all, s_all = gather_blocks(p_own, s_own, rows_n, cols_n)
    product = block_product(codes, counts, p_own, s_own, p_all, s_all)
    return (p_own.reshape(1, 1, p_max, 128, 128), product.reshape(1, 1, q_max, 128, 128))


def solution(mesh):
    return jax.shard_map(
        on_device,
        mesh=mesh,
        in_specs=(
            P("row", None),
            P("row", "col", None),
            P("row", "col"),
            P("row", "col", None, None, None),
            P("row", "col", None),
            P("row", "col"),
            P("row", "col", None),
            P("row", "col"),
        ),
        out_specs=(P("row", "col", None, None, None), P("row", "col", None, None, None)),
        check_vma=False,
    )
```

```python
import functools

import jax
import jax.numpy as jnp
from jax import lax
from jax.experimental import pallas as pl
from jax.experimental.pallas import tpu as pltpu
from jax.sharding import PartitionSpec as P

MESH = pl.DeviceIdType.MESH
MIB = 1 << 20


def rows_kernel(rows_n, cols_n, coeffs, out, send, recv):
    row, col = lax.axis_index("row"), lax.axis_index("col")
    sub = cols_n // rows_n
    height = out.shape[0]
    piece = height // rows_n
    half, share = lax.rem(col, sub), lax.div(col, sub)
    owner = lax.div(col, sub)
    targets = [
        {"row": lax.rem(row + step, rows_n), "col": row * sub + half} for step in range(1, rows_n)
    ]
    sources = [{"row": owner, "col": part * sub + half} for part in range(rows_n)]
    barrier = pltpu.get_barrier_semaphore()
    for device in targets:
        pl.semaphore_signal(barrier, inc=1, device_id=device, device_id_type=MESH)

    @pl.when(row != owner)
    def _():
        for device in sources:
            pl.semaphore_signal(barrier, inc=1, device_id=device, device_id_type=MESH)

    pl.semaphore_wait(barrier, rows_n - 1 + jnp.where(row != owner, rows_n, 0))

    def copy(step, part, device):
        start = half * height + share * piece
        return pltpu.make_async_remote_copy(
            src_ref=coeffs.at[pl.ds(pl.multiple_of(start, piece), piece)],
            dst_ref=out.at[pl.ds(pl.multiple_of(part * piece, piece), piece)],
            send_sem=send.at[step],
            recv_sem=recv.at[part],
            device_id=device,
            device_id_type=MESH,
        )

    sends = [copy(step, share, device) for step, device in enumerate(targets)]
    for one in sends:
        one.start()

    @pl.when(row != owner)
    def _():
        for part, device in enumerate(sources):
            copy(0, part, device).wait_recv()

    for one in sends:
        one.wait_send()


def square_kernel(rows_n, cols_n, parts, coeffs, out, send, recv):
    row, col = lax.axis_index("row"), lax.axis_index("col")
    sub = cols_n // rows_n
    height = out.shape[0]
    size = height // (2 * parts)
    owner = lax.div(col, sub)
    first = lax.rem(col, sub) * height
    y, x = lax.div(row, 2), lax.rem(row, 2)
    dy = lax.rem(y + lax.div(owner, 2), 2)
    dx = lax.rem(x + lax.rem(owner, 2), 2)
    along_x, along_y = y * 2 + 1 - x, (1 - y) * 2 + x
    is_source = row == owner
    sends = [jnp.logical_or(dx == 1, dy == 0), jnp.logical_or(dx == 0, dy == 1)]
    following = [
        jnp.where(dx == dy, along_x, along_y),
        jnp.where(dx == dy, along_y, along_x),
    ]

    barrier = pltpu.get_barrier_semaphore()
    for near in (along_x, along_y):
        pl.semaphore_signal(
            barrier, inc=1, device_id={"row": near, "col": col}, device_id_type=MESH
        )
    pl.semaphore_wait(barrier, 2)

    def copy(way, part, from_input):
        offset = (way * parts + part) * size
        where = out.at[pl.ds(offset, size)]
        start = pl.multiple_of(first + offset, size)
        return pltpu.make_async_remote_copy(
            src_ref=coeffs.at[pl.ds(start, size)] if from_input else where,
            dst_ref=where,
            send_sem=send.at[way, part],
            recv_sem=recv.at[way, part],
            device_id={"row": following[way], "col": col},
            device_id_type=MESH,
        )

    @pl.when(is_source)
    def _():
        for part in range(parts):
            for way in range(2):
                if part >= 2:
                    copy(way, part - 2, True).wait_send()
                copy(way, part, True).start()
        for part in range(max(0, parts - 2), parts):
            for way in range(2):
                copy(way, part, True).wait_send()

    @pl.when(jnp.logical_not(is_source))
    def _():
        for part in range(parts):
            for way in range(2):
                copy(way, part, False).wait_recv()
                pl.when(sends[way])(lambda: copy(way, part, False).start())

    for way in range(2):

        @pl.when(jnp.logical_and(sends[way], jnp.logical_not(is_source)))
        def _():
            for part in range(parts):
                copy(way, part, False).wait_send()


def gather_rows(coeffs, rows_n, cols_n):
    height = coeffs.shape[0] * rows_n // cols_n
    if rows_n == 4:
        parts = max(1, height // 256)
        body = functools.partial(square_kernel, rows_n, cols_n, parts)
        sems = [pltpu.SemaphoreType.DMA((2, parts))] * 2
    else:
        body = functools.partial(rows_kernel, rows_n, cols_n)
        sems = [pltpu.SemaphoreType.DMA((rows_n - 1,)), pltpu.SemaphoreType.DMA((rows_n,))]
    return pl.pallas_call(
        body,
        out_shape=jax.ShapeDtypeStruct((height, coeffs.shape[1]), coeffs.dtype),
        in_specs=[pl.BlockSpec(memory_space=pl.ANY)],
        out_specs=pl.BlockSpec(memory_space=pl.ANY),
        scratch_shapes=sems,
        compiler_params=pltpu.CompilerParams(collective_id=0, has_side_effects=True),
    )(coeffs)


def density_kernel(rows_n, cols_n, ids, count, coeffs, others, out, left, right, sem):
    row, col = lax.axis_index("row"), lax.axis_index("col")
    sub = cols_n // rows_n
    height = others.shape[0]
    tile_cols = height // 128
    load_left = pltpu.make_async_copy(coeffs, left, sem.at[0])
    load_left.start()
    here = row == lax.div(col, sub)
    start = pl.multiple_of(lax.rem(col, sub) * height, height)
    load_own = pltpu.make_async_copy(coeffs.at[pl.ds(start, height)], right, sem.at[1])
    load_other = pltpu.make_async_copy(others, right, sem.at[1])

    @pl.when(here)
    def _():
        load_own.start()

    @pl.when(jnp.logical_not(here))
    def _():
        load_other.start()

    live = count[0]
    load_left.wait()
    load_other.wait()

    def block(slot, carry):
        a = pl.multiple_of(lax.div(ids[slot], tile_cols) * 128, 128)
        b = pl.multiple_of(lax.rem(ids[slot], tile_cols) * 128, 128)
        raw = lax.dot_general(
            left[pl.ds(a, 128), :],
            right[pl.ds(b, 128), :],
            (((1,), (1,)), ((), ())),
            preferred_element_type=jnp.float32,
        )
        out[slot] = raw.astype(out.dtype)
        return carry

    def clear(slot, carry):
        out[slot] = jnp.zeros(out.shape[1:], out.dtype)
        return carry

    lax.fori_loop(0, live, block, 0)
    lax.fori_loop(live, out.shape[0], clear, 0)


def density(ids, count, coeffs, others, rows_n, cols_n):
    slots = ids.shape[0]
    return pl.pallas_call(
        functools.partial(density_kernel, rows_n, cols_n),
        out_shape=jax.ShapeDtypeStruct((slots, 128, 128), jnp.bfloat16),
        in_specs=[pl.BlockSpec(memory_space=pltpu.SMEM)] * 2
        + [pl.BlockSpec(memory_space=pl.ANY)] * 2,
        out_specs=pl.BlockSpec(memory_space=pltpu.VMEM),
        scratch_shapes=[
            pltpu.VMEM(coeffs.shape, coeffs.dtype),
            pltpu.VMEM(others.shape, coeffs.dtype),
            pltpu.SemaphoreType.DMA((2,)),
        ],
        compiler_params=pltpu.CompilerParams(vmem_limit_bytes=40 * MIB),
    )(ids, count, coeffs, others)


def blocks_kernel(rows_n, cols_n, parts, p_own, s_own, p_all, s_all, *sems):
    send, recv, pass_send, pass_recv, s_send, s_recv = sems
    row, col = lax.axis_index("row"), lax.axis_index("col")
    length = cols_n // 2
    z, core = lax.div(col, 2), lax.rem(col, 2)
    size = p_own.shape[0] // parts
    right, left = {"row": row, "col": col + 2}, {"row": row, "col": col - 2}
    partner = {"row": row, "col": z * 2 + 1 - core}
    column = [{"row": lax.rem(row + step, rows_n), "col": col} for step in range(1, rows_n)]
    has_right, has_left = z + 1 < length, z > 0

    barrier = pltpu.get_barrier_semaphore()

    def greet(device):
        pl.semaphore_signal(barrier, inc=1, device_id=device, device_id_type=MESH)

    greet(partner)
    for device in column:
        greet(device)

    @pl.when(has_right)
    def _():
        greet(right)

    @pl.when(has_left)
    def _():
        greet(left)

    pl.semaphore_wait(barrier, rows_n + jnp.where(has_right, 1, 0) + jnp.where(has_left, 1, 0))

    def remote(src, dst, send_sem, recv_sem, device):
        return pltpu.make_async_remote_copy(
            src_ref=src,
            dst_ref=dst,
            send_sem=send_sem,
            recv_sem=recv_sem,
            device_id=device,
            device_id_type=MESH,
        )

    def piece(source, lane, part):
        return p_all.at[source * 2 + lane, pl.ds(part * size, size)]

    def origin(way, step):
        return z - step if way == 0 else z + step

    def sent(way, step, part):
        where = piece(origin(way, step), core, part)
        src = p_own.at[pl.ds(part * size, size)] if step == 0 else where
        device = right if way == 0 else left
        return remote(src, where, send.at[way, step, part], recv.at[way, step, part], device)

    def passed(way, step, part):
        where = piece(origin(way, step), core, part)
        src = p_own.at[pl.ds(part * size, size)] if step == 0 else where
        return remote(
            src, where, pass_send.at[way, step, part], pass_recv.at[way, step, part], partner
        )

    def onward(way):
        return has_right if way == 0 else has_left

    def exists(way, step):
        return z >= step if way == 0 else z + step < length

    for part in range(parts):
        for way in range(2):
            pl.when(onward(way))(lambda way=way: sent(way, 0, part).start())
    s_sends = [
        remote(s_own, s_all.at[row], s_send.at[n], s_recv.at[n], device)
        for n, device in enumerate(column)
    ]
    for one in s_sends:
        one.start()
    for part in range(parts):
        passed(0, 0, part).start()
    for step in range(1, length):
        for part in range(parts):
            for way in range(2):

                @pl.when(exists(way, step))
                def _():
                    sent(way, step - 1, part).wait_recv()
                    passed(way, step, part).start()
                    if step < length - 1:
                        pl.when(onward(way))(lambda: sent(way, step, part).start())

    for part in range(parts):
        passed(0, 0, part).wait()
        for way in range(2):
            pl.when(onward(way))(lambda way=way: sent(way, 0, part).wait_send())
    for step in range(1, length):
        for part in range(parts):
            for way in range(2):

                @pl.when(exists(way, step))
                def _():
                    passed(way, step, part).wait()
                    if step < length - 1:
                        pl.when(onward(way))(lambda: sent(way, step, part).wait_send())

    for one in s_sends:
        one.wait()


def gather_blocks(p_own, s_own, rows_n, cols_n):
    parts = 4 if p_own.shape[0] % 4 == 0 else 1
    table = pltpu.SemaphoreType.DMA((2, cols_n // 2, parts))
    return pl.pallas_call(
        functools.partial(blocks_kernel, rows_n, cols_n, parts),
        out_shape=(
            jax.ShapeDtypeStruct((cols_n,) + p_own.shape, p_own.dtype),
            jax.ShapeDtypeStruct((rows_n,) + s_own.shape, s_own.dtype),
        ),
        in_specs=[pl.BlockSpec(memory_space=pl.ANY)] * 2,
        out_specs=[pl.BlockSpec(memory_space=pl.ANY)] * 2,
        scratch_shapes=[table] * 4 + [pltpu.SemaphoreType.DMA((rows_n - 1,))] * 2,
        compiler_params=pltpu.CompilerParams(collective_id=1, has_side_effects=True),
    )(p_own, s_own)


def product_kernel(rows_n, cols_n, codes, counts, p_own, s_own, p_all, s_all, out, left, right, sem):
    row, col = lax.axis_index("row"), lax.axis_index("col")
    p_max, s_max = p_own.shape[0], s_own.shape[0]
    base = rows_n * s_max
    loads = [pltpu.make_async_copy(p_own, left.at[pl.ds(col * p_max, p_max)], sem.at[0])]
    loads += [pltpu.make_async_copy(s_own, right.at[pl.ds(row * s_max, s_max)], sem.at[1])]
    for step in range(1, cols_n):
        at = lax.rem(col + step, cols_n)
        loads += [
            pltpu.make_async_copy(
                p_all.at[at], left.at[pl.ds(at * p_max, p_max)], sem.at[len(loads)]
            )
        ]
    for step in range(1, rows_n):
        at = lax.rem(row + step, rows_n)
        loads += [
            pltpu.make_async_copy(
                s_all.at[at], right.at[pl.ds(at * s_max, s_max)], sem.at[len(loads)]
            )
        ]
    for load in loads:
        load.start()
    for load in loads:
        load.wait()

    def slot(q, carry):
        def term(n, total):
            code = codes[q, n]
            return total + jnp.dot(
                left[lax.div(code, base)],
                right[lax.rem(code, base)],
                preferred_element_type=jnp.float32,
            )

        out[q] = lax.fori_loop(0, counts[q], term, jnp.zeros((128, 128), jnp.float32))
        return carry

    lax.fori_loop(0, out.shape[0], slot, 0)


def block_product(codes, counts, p_own, s_own, p_all, s_all):
    cols_n, p_max = p_all.shape[:2]
    rows_n, s_max = s_all.shape[:2]
    return pl.pallas_call(
        functools.partial(product_kernel, rows_n, cols_n),
        out_shape=jax.ShapeDtypeStruct((counts.shape[0], 128, 128), jnp.float32),
        in_specs=[pl.BlockSpec(memory_space=pltpu.SMEM)] * 2
        + [pl.BlockSpec(memory_space=pl.ANY)] * 4,
        out_specs=pl.BlockSpec(memory_space=pltpu.VMEM),
        scratch_shapes=[
            pltpu.VMEM((cols_n * p_max, 128, 128), p_all.dtype),
            pltpu.VMEM((rows_n * s_max, 128, 128), s_all.dtype),
            pltpu.SemaphoreType.DMA((cols_n + rows_n,)),
        ],
        compiler_params=pltpu.CompilerParams(vmem_limit_bytes=40 * MIB),
    )(codes, counts, p_own, s_own, p_all, s_all)


def match_lists(p_codes, s_codes, q_ids, q_live, tile_cols, span):
    cols_n, p_max = p_codes.shape
    rows_n, s_max = s_codes.shape
    q_row, q_col = q_ids // tile_cols, q_ids % tile_cols
    at = jnp.arange(tile_cols, dtype=jnp.int32)
    p_want = q_row[:, None] * tile_cols + at[None, :]
    p_hit = p_codes[None, :, None, :] == p_want[:, None, :, None]
    p_slot = jnp.arange(cols_n * p_max, dtype=jnp.int32).reshape(1, cols_n, 1, p_max)
    p_at = jnp.max(jnp.where(p_hit, p_slot, -1), axis=3)
    level = jnp.arange(span * tile_cols, dtype=jnp.int32).reshape(span, tile_cols)
    s_want = level[None] * tile_cols + q_col[:, None, None]
    s_hit = s_codes[None, None, :, None, :] == s_want[:, :, None, :, None]
    s_slot = jnp.arange(rows_n * s_max, dtype=jnp.int32).reshape(1, 1, rows_n, 1, s_max)
    s_at = jnp.max(jnp.where(s_hit, s_slot, -1), axis=4)
    p_at = p_at.reshape(q_ids.shape[0], -1)
    s_at = s_at.reshape(q_ids.shape[0], -1)
    depth = p_at.shape[1]
    match = (p_at >= 0) & (s_at >= 0) & q_live[:, None]
    code = jnp.where(match, p_at * (rows_n * s_max) + s_at, 0)
    order = jnp.arange(depth, dtype=jnp.int32)
    before = order[None, :, None] > order[None, None, :]
    rank = jnp.sum((before & match[:, None, :]).astype(jnp.int32), axis=2)
    rank = jnp.where(match, rank, -1)
    picked = rank[:, None, :] == order[None, :, None]
    codes = jnp.sum(jnp.where(picked, code[:, None, :], 0), axis=2)
    return codes, jnp.sum(match.astype(jnp.int32), axis=1)


def on_device(coeffs, p_slots, p_count, s_blocks, s_slots, s_count, q_slots, q_count):
    rows_n = lax.axis_size("row")
    cols_n = lax.axis_size("col")
    tile_cols = coeffs.shape[0] * rows_n // cols_n // 128
    p_ids, s_ids, q_ids = p_slots[0, 0], s_slots[0, 0], q_slots[0, 0]
    s_own = s_blocks[0, 0]
    p_max, s_max, q_max = p_ids.shape[0], s_ids.shape[0], q_ids.shape[0]

    def live(ids, count):
        return jnp.arange(ids.shape[0], dtype=jnp.int32) < count[0, 0]

    p_codes = lax.all_gather(jnp.where(live(p_ids, p_count), p_ids, -1), "col")
    s_codes = lax.all_gather(jnp.where(live(s_ids, s_count), s_ids, -1), "row")
    codes, counts = match_lists(
        p_codes, s_codes, q_ids, live(q_ids, q_count), tile_cols, cols_n // rows_n
    )
    others = gather_rows(coeffs, rows_n, cols_n)
    p_own = density(p_ids, p_count[0], coeffs, others, rows_n, cols_n)
    p_all, s_all = gather_blocks(p_own, s_own, rows_n, cols_n)
    product = block_product(codes, counts, p_own, s_own, p_all, s_all)
    return (p_own.reshape(1, 1, p_max, 128, 128), product.reshape(1, 1, q_max, 128, 128))


def solution(mesh):
    return jax.shard_map(
        on_device,
        mesh=mesh,
        in_specs=(
            P("row", None),
            P("row", "col", None),
            P("row", "col"),
            P("row", "col", None, None, None),
            P("row", "col", None),
            P("row", "col"),
            P("row", "col", None),
            P("row", "col"),
        ),
        out_specs=(P("row", "col", None, None, None), P("row", "col", None, None, None)),
        check_vma=False,
    )
```
